32 devices in a mesh: parts: 1, var: 8 (over z, core), patch: 4 (over y, x).
Axes of the slice: x: 2, y: 2, z: 4, core: 2. Of those that a mesh axis runs over, the one named last changes fastest.
Arguments:
- tokens: bfloat16 [256, 24, 768], P('patch', ('parts', 'var')), may hold values from -6 to 6
- patch_mask: int32 [256, 24], P('patch', ('parts', 'var')), may hold values 0 or 1
- group_ids: int32 [24], P('parts'), may hold values from 0 to 7, never falling along the last dimension, each value on 1 to 6 neighbouring positions
- time_gain: float32 [768], replicated, may hold values from 0.1 to 1.9
- time_qkv: bfloat16 [768, 3, 768], P(None, None, 'patch'), may hold values from -0.21875 to 0.21875
- time_out: bfloat16 [768, 768], P('patch'), may hold values from -0.21875 to 0.21875
- space_gain: float32 [768], replicated, may hold values from 0.1 to 1.9
- space_qkv: bfloat16 [768, 3, 768], P(None, None, 'patch'), may hold values from -0.21875 to 0.21875
- space_out: bfloat16 [768, 768], P('patch'), may hold values from -0.21875 to 0.21875
Outputs:
- panel_out: bfloat16 [256, 24, 768], P('patch', ('parts', 'var'))
The draws below stay inside these ranges and needn't reach their ends.
Inputs may be any that keep to these rules, and one draw needn't show every extreme that they name: group_ids never falls along the variates; each group is a run of 1 to 6 consecutive variates.
All inputs are finite; a program needn't handle non-finite values. No bound on the sum of `patch_mask` on one device may be relied on, other than what follows from the above.
Results may differ from the reference program's by a relative error of at most 0.017.
Values may be sent and summed in bfloat16 or wider, within the bound.
A program may use at most 64 MiB of HBM per device.

```python
import math
import jax
import jax.numpy as jnp
import numpy as np
from jax import lax

D = 768
HEADS = 12
HD = 64
VAR_DEV = 3
V = 24
P_SIZE = 256
GMAX = 6
GROUPS = 8
N_PATCH = 4


def plant(result, key, low, top_value):
    extent = result.shape
    place = [jax.random.randint(jax.random.fold_in(key, axis), (), 0, extent[axis]) for axis in range(len(extent))]
    result = result.at[tuple(place)].set(low)
    longest = extent.index(max(extent))
    place[longest] = (place[longest] + 1) % extent[longest]
    return result.at[tuple(place)].set(top_value)


def block_levels(key, shape, cuts, least, largest):
    factor_of = 1.0
    for dim, blocks in cuts:
        draws = jax.random.uniform(jax.random.fold_in(jax.random.fold_in(key, 6), dim), (blocks,), jnp.float32, least / len(cuts), largest / len(cuts))
        factor_of = factor_of * jnp.repeat(jnp.exp(draws), shape[dim] // blocks).reshape((-1,) + (1,) * (len(shape) - 1 - dim))
    return factor_of


def split_up(number_of, total, limit, skew):
    weights = [(1 << 20) // math.isqrt(grade ** skew) + 1 for grade in range(2, number_of + 1)]
    surplus, holding = total - limit - (number_of - 1), [1] * (number_of - 1)
    while surplus > 0:
        movable = [i for i in range(number_of - 1) if holding[i] < limit]
        mass, remaining = sum([weights[i] for i in movable]), surplus
        for i in movable:
            more = min(limit - holding[i], max(1, remaining * weights[i] // mass), surplus)
            holding[i] = holding[i] + more
            surplus = surplus - more
    return np.array([limit] + holding)


def uneven(own_key, count, total, limit, skew):
    if count == 2:
        one = jax.random.randint(own_key, (), max(1, total - limit), min(limit, total - 1) + 1)
        return jnp.stack([one, total - one])
    lengths = jnp.asarray(split_up(count, total, limit, skew), jnp.int32)
    twos = (count - 1) // 2
    source_of, receiver = lengths[1:1 + 2 * twos:2], lengths[2:2 + 2 * twos:2]
    slack = jnp.minimum(source_of - 1, limit - receiver)
    shifted = jax.random.randint(jax.random.fold_in(own_key, 1), (twos,), 0, 1 << 20) % (slack + 1)
    lengths = lengths.at[1:1 + 2 * twos:2].set(source_of - shifted).at[2:2 + 2 * twos:2].set(receiver + shifted)
    return lengths[jax.random.permutation(jax.random.fold_in(own_key, 2), count)]


def normal_values(key, extent, deviation, limit, cuts=(), kind=jnp.bfloat16):
    level = block_levels(key, extent, cuts, -0.22, 0.18) if cuts else 1.0
    array = jax.random.normal(key, extent, jnp.float32) * deviation * level
    return jnp.minimum(jnp.maximum(array, -limit), limit).astype(kind)


def setup_inputs(seed: int = 0, part: int = 0) -> dict:
    keys = jax.random.split(jax.random.key(seed), 10)
    part_keys = jax.random.split(jax.random.fold_in(keys[9], part), 10)
    tokens = normal_values(part_keys[0], (P_SIZE, V, D), 1.0, 6.0, ((0, 4), (1, 8)))
    patch_mask = plant((jax.random.randint(part_keys[1], (P_SIZE, V), 0, 4) < 3).astype(jnp.int32), jax.random.fold_in(part_keys[1], 1), 0, 1)
    group_ids = jnp.searchsorted(jnp.cumsum(uneven(part_keys[2], GROUPS, V, GMAX, 2)), jnp.arange(V), side="right").astype(jnp.int32)
    time_gain = jnp.clip(1.0 + 0.18 * jax.random.normal(keys[3], (D,), jnp.float32), 0.1, 1.9)
    time_qkv = normal_values(keys[4], (D, 3, D), D ** -0.5, 0.21875, ((2, 4),))
    time_out = normal_values(keys[5], (D, D), D ** -0.5, 0.21875, ((0, 4),))
    space_gain = jnp.clip(1.0 + 0.18 * jax.random.normal(keys[6], (D,), jnp.float32), 0.1, 1.9)
    space_qkv = normal_values(keys[7], (D, 3, D), D ** -0.5, 0.21875, ((2, 4),))
    space_out = normal_values(keys[8], (D, D), D ** -0.5, 0.21875, ((0, 4),))
    return {"tokens": tokens, "patch_mask": patch_mask, "group_ids": group_ids, "time_gain": time_gain, "time_qkv": time_qkv, "time_out": time_out, "space_gain": space_gain, "space_qkv": space_qkv, "space_out": space_out}


epsilon = 1e-06

def norm_rows(block_rows, gain):
    floats = block_rows.astype(jnp.float32)
    scaled = floats * lax.rsqrt(lax.optimization_barrier(jnp.mean(floats * floats, axis=-1, keepdims=True)) + epsilon)
    return (scaled * gain.astype(jnp.float32)).astype(jnp.bfloat16)

def project(normed, weight):
    return jnp.einsum('pvd,dtk->pvtk', normed.astype(jnp.float32), weight.astype(jnp.float32)).astype(jnp.bfloat16)

def soft_weights(scores, allowed):
    masked = jnp.where(allowed, scores, -jnp.inf)
    highest = lax.optimization_barrier(jnp.max(masked, axis=-1, keepdims=True))
    raised = jnp.exp(masked - highest)
    return (raised / lax.optimization_barrier(jnp.sum(raised, axis=-1, keepdims=True))).astype(jnp.bfloat16)

def head_sum(attended, weight):
    group_width = D // N_PATCH
    lead_shape = attended.shape[:-1]
    flat = attended.reshape(-1, D)
    summed = jnp.zeros((flat.shape[0], D), jnp.float32)
    for group in range(N_PATCH):
        part = jnp.dot(flat[:, group * group_width:(group + 1) * group_width], weight[group * group_width:(group + 1) * group_width], preferred_element_type=jnp.float32)
        part = lax.optimization_barrier(part.astype(jnp.bfloat16))
        summed = summed + part.astype(jnp.float32)
    return summed.reshape(lead_shape + (D,))

def time_block(block_rows, block_mask, gain, weight, out_weight):
    patch_count, var_count = (block_rows.shape[0], block_rows.shape[1])
    projected = project(norm_rows(block_rows, gain), weight)
    queries = projected[:, :, 0].reshape(patch_count, var_count, HEADS, HD).astype(jnp.float32)
    key_rows = projected[:, :, 1].reshape(patch_count, var_count, HEADS, HD).astype(jnp.float32)
    value_rows = projected[:, :, 2].reshape(patch_count, var_count, HEADS, HD).astype(jnp.float32)
    scores = jnp.einsum('qvhe,kvhe->vhqk', queries, key_rows) * HD ** (-0.5)
    query_pos = jnp.arange(patch_count)[:, None]
    key_pos = jnp.arange(patch_count)[None, :]
    observed = (block_mask.T > 0)[:, None, None, :]
    allowed = (key_pos <= query_pos)[None, None] & (observed | (key_pos == query_pos)[None, None])
    weights = soft_weights(scores, allowed)
    attended = jnp.einsum('vhqk,kvhe->qvhe', weights.astype(jnp.float32), value_rows).astype(jnp.bfloat16)
    attended = attended.reshape(patch_count, var_count, D)
    mixed = head_sum(attended, out_weight)
    return (block_rows.astype(jnp.float32) + mixed).astype(jnp.bfloat16)

def space_block(block_rows, group_ids, gain, weight, out_weight):
    patch_count, var_count = (block_rows.shape[0], block_rows.shape[1])
    projected = project(norm_rows(block_rows, gain), weight)
    queries = projected[:, :, 0].reshape(patch_count, var_count, HEADS, HD).astype(jnp.float32)
    key_rows = projected[:, :, 1].reshape(patch_count, var_count, HEADS, HD).astype(jnp.float32)
    value_rows = projected[:, :, 2].reshape(patch_count, var_count, HEADS, HD).astype(jnp.float32)
    scores = jnp.einsum('pqhe,pkhe->phqk', queries, key_rows) * HD ** (-0.5)
    allowed = (group_ids[:, None] == group_ids[None, :])[None, None]
    weights = soft_weights(scores, allowed)
    attended = jnp.einsum('phqk,pkhe->pqhe', weights.astype(jnp.float32), value_rows).astype(jnp.bfloat16)
    attended = attended.reshape(patch_count, var_count, D)
    mixed = head_sum(attended, out_weight)
    return (block_rows.astype(jnp.float32) + mixed).astype(jnp.bfloat16)

def reference(tokens, patch_mask, group_ids, time_gain, time_qkv, time_out, space_gain, space_qkv, space_out):
    block_count = V // VAR_DEV

    def time_step(block):
        start = (block * VAR_DEV).astype(jnp.int32)
        rows_in = lax.dynamic_slice_in_dim(tokens, start, VAR_DEV, 1)
        mask_in = lax.dynamic_slice_in_dim(patch_mask, start, VAR_DEV, 1)
        return time_block(rows_in, mask_in, time_gain, time_qkv, time_out)
    middle = lax.map(time_step, jnp.arange(block_count, dtype=jnp.int32))
    middle = jnp.transpose(middle, (1, 0, 2, 3)).reshape(P_SIZE, V, D)
    patch_blocks = P_SIZE // N_PATCH

    def space_step(block):
        start = (block * N_PATCH).astype(jnp.int32)
        rows_in = lax.dynamic_slice_in_dim(middle, start, N_PATCH, 0)
        return space_block(rows_in, group_ids, space_gain, space_qkv, space_out)
    final = lax.map(space_step, jnp.arange(patch_blocks, dtype=jnp.int32))
    return final.reshape(P_SIZE, V, D)
```

```python
import functools

import jax
import jax.numpy as jnp
from jax import lax
from jax.experimental import pallas as pl
from jax.experimental.pallas import tpu as pltpu
from jax.sharding import PartitionSpec as P

HD = 64
REACH = 5
EPS = 1e-06
MESH = pl.DeviceIdType.MESH
F32 = jnp.float32
BF16 = jnp.bfloat16


def norm_rows(rows, gain):
    floats = rows.astype(F32)
    scaled = floats * lax.rsqrt(jnp.mean(floats * floats, axis=-1, keepdims=True) + EPS)
    return (scaled * gain).astype(BF16)


def dot(a, b):
    return jnp.dot(a, b, preferred_element_type=F32)


def dot_t(a, b):
    return lax.dot_general(a, b, (((1,), (1,)), ((), ())), preferred_element_type=F32)


def kernel(
    n, nvar, tok, marks, gids, tgain, sgain, wt_in, wot_in, wqs_in, wos_in,
    out, gx, mk, wt, wot, wqs, wos, att, ratt, mid, sw, kvb, qb, prod, sc, pb,
    local_sem, tok_s, tok_r, mk_s, mk_r, w_s, w_r, att_s, att_r, win_s, win_r,
):
    me = lax.axis_index("patch")
    var = lax.axis_index("var")
    nv, pp, dm = tok.shape
    hw = wot_in.shape[0]
    heads = hw // HD
    side = (me + 1 - 2 * (me % 2), me + 2 - 4 * ((me // 2) % 2), n - 1 - me)
    sib = var + 1 - 2 * (var % 2)
    core = var % 2
    nbrs = (1, -1, 2, -2)

    def exists(k):
        return (var + k >= 0) & (var + k < nvar)

    barrier = pltpu.get_barrier_semaphore()
    count = n - 1 + 1
    for other in side:
        pl.semaphore_signal(barrier, inc=1, device_id={"patch": other}, device_id_type=MESH)
    pl.semaphore_signal(barrier, inc=1, device_id={"var": sib}, device_id_type=MESH)
    for k in nbrs:
        @pl.when(exists(k))
        def _():
            pl.semaphore_signal(barrier, inc=1, device_id={"var": var + k}, device_id_type=MESH)
        count = count + exists(k).astype(jnp.int32)
    own = [
        pltpu.make_async_copy(wot_in, wot.at[me], local_sem.at[0]),
        pltpu.make_async_copy(wqs_in, wqs.at[me], local_sem.at[1]),
        pltpu.make_async_copy(wos_in, wos.at[me], local_sem.at[2]),
        pltpu.make_async_copy(wt_in, wt, local_sem.at[3]),
        pltpu.make_async_copy(tok, gx.at[:, pl.ds(pl.multiple_of(me * pp, pp), pp), :], local_sem.at[4]),
    ]
    for i in (4, 3, 0, 1, 2):
        own[i].start()
    pl.semaphore_wait(barrier, count)

    sends = []

    def remote(src, dst, ssem, rsem, **where):
        c = pltpu.make_async_remote_copy(
            src_ref=src, dst_ref=dst, send_sem=ssem, recv_sem=rsem, device_id=where, device_id_type=MESH
        )
        return c

    def launch(*a, **k):
        c = remote(*a, **k)
        c.start()
        sends.append(c)
        return c

    def block(of, lo=0, num=pp):
        return pl.ds(pl.multiple_of(of * pp + lo, num), num)

    half = pp // 2
    mk_c = [launch(marks, mk.at[me], mk_s.at[d], mk_r.at[d], patch=side[d]) for d in range(3)]
    tok_c = {}
    for i in range(nv):
        for d in (0, 1):
            v = i if d == 1 else nv - 1 - i
            tok_c[d, v] = launch(tok.at[v], gx.at[v, block(me), :], tok_s.at[d, v], tok_r.at[d, v], patch=side[d])
    routes = ((1, 0, 0, pp), (0, 2, 0, pp), (1, 1, 0, half), (0, 1, half, half))
    diag_c = []
    for i, (d, v, lo, num) in enumerate(routes):
        tok_c[d, v].wait_recv()
        piece = gx.at[v, block(side[d], lo, num), :]
        diag_c.append(launch(piece, piece, tok_s.at[2, i], tok_r.at[2, i], patch=side[1 - d]))

    arrays = ((wot_in, wot), (wqs_in, wqs), (wos_in, wos))
    wc = {}

    def piece_of(a, shard, part=None):
        rows = arrays[a][1].shape[1] // 2
        if part is None:
            return arrays[a][1].at[shard, pl.ds(pl.multiple_of(core * rows, rows), rows), :]
        num = rows // 2
        return arrays[a][1].at[shard, pl.ds(pl.multiple_of(core * rows + part * num, num), num), :]

    def w_own(a):
        src = arrays[a][0]
        rows = src.shape[0] // 2
        for d in (0, 1):
            wc[a, d] = launch(
                src.at[pl.ds(pl.multiple_of(core * rows, rows), rows), :], piece_of(a, me),
                w_s.at[a, d], w_r.at[a, d], patch=side[d],
            )

    def w_relay(a):
        for d in (0, 1):
            wc[a, d].wait_recv()
            piece = piece_of(a, side[d], 1 - d)
            wc[a, 2 + d] = launch(piece, piece, w_s.at[a, 2 + d], w_r.at[a, 2 + d], patch=side[1 - d])
            piece = piece_of(a, side[d])
            wc[a, 4 + d] = launch(piece, piece, w_s.at[a, 4 + d], w_r.at[a, 4 + d], var=sib)

    def w_diag(a):
        wc[a, 2].wait_recv()
        wc[a, 3].wait_recv()
        piece = piece_of(a, side[2])
        wc[a, 6] = launch(piece, piece, w_s.at[a, 6], w_r.at[a, 6], var=sib)

    w_own(0)
    w_own(2)
    for k in nbrs:
        lo = {1: 9, -1: 3, 2: 12, -2: 1}[k]
        num = nv if abs(k) == 1 else nv - 1

        @pl.when(jnp.logical_not(exists(k)))
        def _():
            sw[lo:lo + num] = jnp.zeros((num, pp, dm), BF16)

    mk[me] = marks[...]
    own[3].wait()
    own[4].wait()
    for c in mk_c:
        c.wait_recv()
    for d in (0, 1):
        for v in range(nv):
            if (d, v) not in [r[:2] for r in routes]:
                tok_c[d, v].wait_recv()
    for c in diag_c:
        c.wait_recv()

    full = n * pp
    seen = jnp.concatenate([mk[s] for s in range(n)], axis=1)
    qi = lax.broadcasted_iota(jnp.int32, (full, full), 0)
    ki = lax.broadcasted_iota(jnp.int32, (full, full), 1)
    att_c = []
    for v in range(nv):
        normed = norm_rows(gx[v], tgain[...])
        proj = dot_t(normed, wt[...]).astype(BF16)
        allowed = ((ki < qi) & (seen[v:v + 1, :] > 0)) | (ki == qi)
        outs = []
        for h in range(heads):
            q = proj[:, h * HD:(h + 1) * HD]
            k = proj[:, hw + h * HD:hw + (h + 1) * HD]
            val = proj[:, 2 * hw + h * HD:2 * hw + (h + 1) * HD]
            s = lax.dot_general(q, k, (((1,), (1,)), ((), ())), preferred_element_type=F32) * HD ** (-0.5)
            s = jnp.where(allowed, s, -jnp.inf)
            e = jnp.exp(s - jnp.max(s, axis=-1, keepdims=True))
            w = (e / jnp.sum(e, axis=-1, keepdims=True)).astype(BF16)
            outs.append(dot(w, val).astype(BF16))
        att[v] = jnp.concatenate(outs, axis=1)
        for d in (2, 0, 1):
            att_c.append(launch(att.at[v, block(side[d]), :], ratt.at[me, v], att_s.at[v, d], att_r.at[v, d], patch=side[d]))
        ratt[me, v] = att[v, block(me), :]
    w_relay(0)
    w_own(1)
    own[0].wait()
    for c in att_c:
        c.wait_recv()
    w_diag(0)
    for k in (4, 5, 6):
        wc[0, k].wait_recv()

    rows = nv * pp
    mix = jnp.zeros((rows, dm), F32)
    for s in range(n):
        mix = mix + dot(ratt[s].reshape(rows, hw), wot[s]).astype(BF16).astype(F32)
    middle = (gx[:, block(me), :].reshape(rows, dm).astype(F32) + mix).astype(BF16)
    mid[...] = middle
    sw[6:6 + nv] = norm_rows(middle, sgain[...]).reshape(nv, pp, dm)

    def window(k, i):
        src = {1: (6, 9), -1: (6, 9), 2: (7, 9), -2: (6, 8)}[k]
        dst = {1: (3, 6), -1: (9, 12), 2: (1, 3), -2: (12, 14)}[k]
        return remote(sw.at[src[0]:src[1]], sw.at[dst[0]:dst[1]], win_s.at[i], win_r.at[i], var=var + k)

    for i, k in enumerate(nbrs):
        @pl.when(exists(k))
        def _():
            window(k, i).start()

    own[1].wait()
    own[2].wait()
    w_relay(1)
    w_relay(2)
    for i, k in enumerate(nbrs):
        @pl.when(exists(-k))
        def _():
            window(k, i).wait_recv()

    nkey = 4 + 3 * nv
    pairs = [(u, u + 6 + t) for u in range(nv) for t in range(-REACH, REACH + 1)]
    sc[...] = jnp.zeros_like(sc)

    def scores_of(s):
        qb[...] = dot_t(sw[6:6 + nv].reshape(rows, dm), wqs[s, :hw, :]).astype(BF16).reshape(nv, pp, hw)
        kvb[s] = dot_t(sw[1:1 + nkey].reshape(nkey * pp, dm), wqs[s, hw:, :]).astype(BF16).reshape(nkey, pp, 2 * hw)
        for i, (u, j) in enumerate(pairs):
            prod[i * pp:(i + 1) * pp, :] = (
                qb[u].astype(F32) * kvb[s, j - 1, :, :hw].astype(F32)
            ).astype(BF16)
        lane = lax.broadcasted_iota(jnp.int32, (hw, 128), 0) // HD + heads * s
        col = lax.broadcasted_iota(jnp.int32, (hw, 128), 1)
        sc[...] += dot(prod[...], (lane == col).astype(F32).astype(BF16))

    def soften():
        total = gids.shape[0]
        local_n = total // nv
        base = (var % local_n) * nv
        for u in range(nv):
            mine_group = gids[base + u]
            slabs = []
            for t in range(-REACH, REACH + 1):
                w = base + u + t
                inside = (w >= 0) & (w < total)
                at = jnp.minimum(jnp.maximum(w, 0), total - 1)
                i = pairs.index((u, u + 6 + t))
                ok = inside & (gids[at] == mine_group)
                slabs.append(jnp.where(ok, sc[i * pp:(i + 1) * pp, :] * HD ** (-0.5), -jnp.inf))
            top = functools.reduce(jnp.maximum, slabs)
            es = [jnp.exp(x - top) for x in slabs]
            den = functools.reduce(lambda a, b: a + b, es)
            for t, e in enumerate(es):
                i = u * (2 * REACH + 1) + t
                pb[i * pp:(i + 1) * pp, :] = (e / den).astype(BF16)

    def mix_of(s):
        lane = lax.broadcasted_iota(jnp.int32, (128, hw), 1) // HD + heads * s
        col = lax.broadcasted_iota(jnp.int32, (128, hw), 0)
        spread = (lane == col).astype(F32).astype(BF16)
        done = []
        for u in range(nv):
            total_u = jnp.zeros((pp, hw), F32)
            lo = u * (2 * REACH + 1)
            wide = dot(pb[lo * pp:(lo + 2 * REACH + 1) * pp, :], spread)
            for t in range(2 * REACH + 1):
                val = kvb[s, u + t, :, hw:].astype(F32)
                total_u = total_u + wide[t * pp:(t + 1) * pp] * val
            done.append(total_u.astype(BF16))
        res = dot(jnp.concatenate(done, axis=0), wos[s]).astype(BF16).astype(F32)
        return res

    scores_of(me)
    for d in (0, 1):
        wc[1, 4 + d].wait_recv()
        scores_of(side[d])
    w_diag(1)
    soften()
    mix2 = mix_of(me)
    for d in (0, 1):
        wc[2, 4 + d].wait_recv()
        mix2 = mix2 + mix_of(side[d])
    w_diag(2)
    wc[1, 6].wait_recv()
    scores_of(side[2])
    soften()
    wc[2, 6].wait_recv()
    mix2 = mix2 + mix_of(side[2])
    out[...] = (mid[...].astype(F32) + mix2).astype(BF16).reshape(nv, pp, dm)

    for c in sends:
        c.wait_send()
    for i, k in enumerate(nbrs):
        @pl.when(exists(k))
        def _():
            window(k, i).wait_send()


def on_device(n, nvar, tokens, patch_mask, group_ids, time_gain, time_qkv, time_out, space_gain, space_qkv, space_out):
    pp, nv, dm = tokens.shape
    hw = time_out.shape[0]
    tok = jnp.transpose(tokens, (1, 0, 2))
    wt = jnp.transpose(time_qkv, (1, 2, 0)).reshape(3 * hw, dm)
    wqs = jnp.transpose(space_qkv, (1, 2, 0)).reshape(3 * hw, dm)
    npair = nv * (2 * REACH + 1)
    vm = pl.BlockSpec(memory_space=pltpu.VMEM)
    anyv = pl.BlockSpec(memory_space=pltpu.HBM)
    dma = pltpu.SemaphoreType.DMA
    res = pl.pallas_call(
        functools.partial(kernel, n, nvar),
        out_shape=jax.ShapeDtypeStruct((nv, pp, dm), BF16),
        in_specs=[anyv, vm, pl.BlockSpec(memory_space=pltpu.SMEM), vm, vm, anyv, anyv, anyv, anyv],
        out_specs=vm,
        scratch_shapes=[
            pltpu.VMEM((nv, n * pp, dm), BF16),
            pltpu.VMEM((n, nv, pp), jnp.int32),
            pltpu.VMEM((3 * hw, dm), BF16),
            pltpu.VMEM((n, hw, dm), BF16),
            pltpu.VMEM((n, 3 * hw, dm), BF16),
            pltpu.VMEM((n, hw, dm), BF16),
            pltpu.VMEM((nv, n * pp, hw), BF16),
            pltpu.VMEM((n, nv, pp, hw), BF16),
            pltpu.VMEM((nv * pp, dm), BF16),
            pltpu.VMEM((5 * nv, pp, dm), BF16),
            pltpu.VMEM((n, 4 + 3 * nv, pp, 2 * hw), BF16),
            pltpu.VMEM((nv, pp, hw), BF16),
            pltpu.VMEM((npair * pp, hw), BF16),
            pltpu.VMEM((npair * pp, 128), F32),
            pltpu.VMEM((npair * pp, 128), BF16),
            dma((5,)), dma((3, 4)), dma((3, 4)), dma((3,)), dma((3,)),
            dma((3, 7)), dma((3, 7)), dma((nv, 3)), dma((nv, 3)), dma((4,)), dma((4,)),
        ],
        compiler_params=pltpu.CompilerParams(
            collective_id=0, has_side_effects=True, vmem_limit_bytes=40_000_000
        ),
    )(tok, patch_mask.T, group_ids, time_gain, space_gain, wt, time_out, wqs, space_out)
    return jnp.transpose(res, (1, 0, 2))


def solution(mesh):
    in_specs = (
        P("patch", ("parts", "var"), None),
        P("patch", ("parts", "var")),
        P("parts"),
        P(),
        P(None, None, "patch"),
        P("patch", None),
        P(),
        P(None, None, "patch"),
        P("patch", None),
    )
    out_specs = P("patch", ("parts", "var"), None)
    return jax.shard_map(
        functools.partial(on_device, mesh.shape["patch"], mesh.shape["var"]),
        mesh=mesh, in_specs=in_specs, out_specs=out_specs, check_vma=False,
    )
```

```python
import functools

import jax
import jax.numpy as jnp
from jax import lax
from jax.experimental import pallas as pl
from jax.experimental.pallas import tpu as pltpu
from jax.sharding import PartitionSpec as P

HD = 64
REACH = 5
TILE = 16
KEYS = 256
BATCH = 6
EPS = 1e-06
MESH = pl.DeviceIdType.MESH
F32 = jnp.float32
BF16 = jnp.bfloat16

GROUPS = ("q", "k", "v", "ot", "os")
SHARED = ('ot', 'k', 'v')
SPLIT = ()
PLAN = (
    "ot:D", "k:D", "n", "init", "v:D", "t0", "ot:Z", "t2", "v:R", "t1", "v:Z", "tr0",
    "k:Z", "ot:R", "tr2", "v:G", "tr1", "k:R", "c0", "ot:G", "c2", "c1", "q:D", "ot:T",
    "k:G", "ot:U", "m0", "os:D", "k:T", "k:U", "m2", "v:T", "v:U", "m1", "Ak", "Av",
    "q:R", "os:R", "Hk", "Hv", "q:G", "Aq", "S0", "os:G", "S1", "O",
)


def norm_rows(rows, gain):
    floats = rows.astype(F32)
    scaled = floats * lax.rsqrt(jnp.mean(floats * floats, axis=-1, keepdims=True) + EPS)
    return (scaled * gain).astype(BF16)


def dot(a, b):
    return jnp.dot(a, b, preferred_element_type=F32)


def dot_t(a, b):
    return lax.dot_general(a, b, (((1,), (1,)), ((), ())), preferred_element_type=F32)


def sem_names(nv):
    names = ["mk", "near", "far"]
    for v in range(nv):
        names += [("t", v), ("tr", v), ("a", v)]
    for g in GROUPS:
        names += [("w", g), ("wr", g), ("ws", g, 0), ("ws", g, 1)]
        if g in SHARED:
            names += [("wz", g, 0), ("wt", g, 0)]
        if g in SHARED + SPLIT:
            names += [("wz", g, 1), ("wt", g, 1)]
    return {name: i for i, name in enumerate(names + [(w, g) for w in ("ko", "kh") for g in "kv"])}


def kernel(
    n, nvar, tok, marks, gids_in, tgain_in, sgain_in, wt_in, wot_in, wqs_in, wos_in,
    out, gx, raw, mk, wt, wall, att, att_b, ratt, ratt_b, mid, sx, kv, qb, mask, att2,
    gids, tgain, sgain, local_sem, recv, send,
):
    me = lax.axis_index("patch")
    var = lax.axis_index("var")
    nv, pp, dm = tok.shape
    hw = wot_in.shape[0]
    heads = hw // HD
    full = n * pp
    rows = nv * pp
    wide = 2 * HD
    slots = 2 * REACH + nv
    side = (me + 1 - 2 * (me % 2), me + 2 - 4 * ((me // 2) % 2), n - 1 - me)
    order = (me, side[0], side[1], side[2])
    core = var % 2
    sib = var + 1 - 2 * core
    plane = (var // 2) % 2
    mate = var + 2 - 4 * plane
    near = var + 2 * core - 1
    far = var + 2 - 4 * core
    near_ok = (near >= 0) & (near < nvar)
    far_ok = (far >= 0) & (far < nvar)
    own0 = (1 - core) * REACH
    out0 = core * nv
    names = sem_names(nv)

    barrier = pltpu.get_barrier_semaphore()
    count = n - 1
    for other in side:
        pl.semaphore_signal(barrier, inc=1, device_id={"patch": other}, device_id_type=MESH)
    for k in (1, -1, 2, -2):
        there = (var + k >= 0) & (var + k < nvar)

        @pl.when(there)
        def _():
            pl.semaphore_signal(barrier, inc=1, device_id={"var": var + k}, device_id_type=MESH)
        count = count + there.astype(jnp.int32)

    def base(g, shard):
        return (GROUPS.index(g) * n + shard) * hw

    def wrows(g, shard, lo, num, cols=None):
        at = pl.ds(pl.multiple_of(base(g, shard) + lo, 16), num)
        return wall.at[at, :] if cols is None else wall.at[at, pl.ds(cols * (dm // 2), dm // 2)]

    def source(g, lo, num):
        if g == "ot":
            return wot_in.at[pl.ds(pl.multiple_of(lo, 16), num), :]
        if g == "os":
            return wos_in.at[pl.ds(pl.multiple_of(lo, 16), num), :]
        return wqs_in.at[pl.ds(pl.multiple_of(("q", "k", "v").index(g) * hw + lo, 16), num), :]

    def mine(g):
        num = hw // 4 if g in SHARED else hw // 2
        return (2 * plane + core if g in SHARED else core) * num, num

    def part(g, other=0):
        if g not in SHARED + SPLIT:
            return mine(g)
        num = hw // 4
        which = plane if other == 0 else 1 - plane
        return (2 * which + core if g in SHARED else 2 * core + which) * num, num

    def mine_rows(g):
        return wall.at[pl.ds(pl.multiple_of(base(g, me), hw), hw), :]

    own = [
        pltpu.make_async_copy(tok, raw, local_sem.at[0]),
        pltpu.make_async_copy(wt_in, wt, local_sem.at[1]),
    ] + [
        pltpu.make_async_copy(source(g, 0, hw), mine_rows(g), local_sem.at[2 + i]) for i, g in enumerate(GROUPS)
    ] + [
        pltpu.make_async_copy(a, b, local_sem.at[2 + len(GROUPS) + i])
        for i, (a, b) in enumerate(((tgain_in, tgain), (sgain_in, sgain), (gids_in, gids), (marks, mk.at[me])))
    ]
    for i in (0, 2 + len(GROUPS), *range(1, 2 + len(GROUPS)), *range(3 + len(GROUPS), len(own))):
        own[i].start()
    pl.semaphore_wait(barrier, count)

    sent = {"w": 0, "x": 0}
    waited = set()

    def push(kind, src, dst, name, size, **where):
        lane = ("w", "x", "mk", "near", "far").index(kind)
        if kind in sent:
            sent[kind] += size
        pltpu.make_async_remote_copy(
            src_ref=src, dst_ref=dst, send_sem=send.at[lane], recv_sem=recv.at[names[name]],
            device_id=where, device_id_type=MESH,
        ).start()

    def drain(sem, num):
        settle(sem, wall.at[pl.ds(0, num), :])

    def settle(sem, ref):
        pltpu.make_async_copy(ref, ref, sem).wait()

    def need(name, num, ref=None):
        if name not in waited:
            waited.add(name)
            settle(recv.at[names[name]], wall.at[pl.ds(0, num), :] if ref is None else ref)

    def need_own(i):
        if ("own", i) not in waited:
            waited.add(("own", i))
            own[i].wait()

    def block(of, lo=0, num=pp):
        return pl.ds(pl.multiple_of(of * pp + lo, num), num)

    half = pp // 2

    def tokens(v):
        for d in (0, 1):
            piece = gx.at[v, block(me), :]
            push("x", piece, piece, ("t", v), pp, patch=side[d])

    def tokens_relay(v):
        need(("t", v), 2 * pp)
        for d in (0, 1):
            piece = gx.at[v, block(side[1 - d], d * half, half), :]
            push("x", piece, piece, ("tr", v), half, patch=side[d])

    def w_direct(g):
        lo, num = mine(g)
        for d in (0, 1):
            push("w", source(g, lo, num), wrows(g, me, lo, num), ("w", g), num, patch=side[d])

    def w_relay(g):
        lo, num = mine(g)
        need(("w", g), 2 * num)
        low, few = part(g)
        for d in (0, 1):
            piece = wrows(g, side[1 - d], low, few, d)
            push("w", piece, piece, ("wr", g), few // 2, patch=side[d])
        for d in (0, 1):
            piece = wrows(g, side[d], lo, num)
            push("w", piece, piece, ("ws", g, 0), num, var=sib)

    def w_mate(g):
        lo, num = mine(g)
        need(("w", g), 2 * num)
        for d in (0, 1):
            piece = wrows(g, side[d], lo, num)
            push("w", piece, piece, ("wz", g, 0), num, var=mate)

    def w_diag(g):
        lo, num = part(g)
        need(("wr", g), num)
        piece = wrows(g, side[2], lo, num)
        push("w", piece, piece, ("ws", g, 1), num, var=sib)
        if g in SHARED + SPLIT:
            push("w", piece, piece, ("wz", g, 1), num, var=mate)

    def w_share(g, j):
        lo, num = part(g, 1)
        need(("wz", g, j), (2 - j) * num)
        for d in ((0, 1), (2,))[j]:
            piece = wrows(g, side[d], lo, num)
            push("w", piece, piece, ("wt", g, j), num, var=sib)

    def have(g, j):
        if j == 0:
            need_own(2 + GROUPS.index(g))
            return
        i = j // 3
        num = (part(g) if i else mine(g))[1]
        need(("ws", g, i), (2 - i) * num)
        if g in SHARED or (i and g in SPLIT):
            need(("wt", g, i), (2 - i) * num)

    def init():
        need_own(4 + len(GROUPS))
        total = gids.shape[0]
        start = (var % (total // nv)) * nv
        slot = lax.broadcasted_iota(jnp.int32, (TILE, KEYS), 1) // TILE
        same = lax.broadcasted_iota(jnp.int32, (TILE, KEYS), 0) == lax.broadcasted_iota(jnp.int32, (TILE, KEYS), 1) % TILE
        for u in range(nv):
            mine_group = gids[start + u]
            line = jnp.full((TILE, KEYS), -jnp.inf, F32)
            for i in range(slots):
                w = start + i - REACH
                inside = (w >= 0) & (w < total)
                at = jnp.minimum(jnp.maximum(w, 0), total - 1)
                ok = jnp.where(inside & (gids[at] == mine_group), 0.0, -jnp.inf).astype(F32)
                line = jnp.where(slot == i, ok, line)
            mask[u * TILE:(u + 1) * TILE] = jnp.where(same, line, -jnp.inf)

        @pl.when(jnp.logical_not(near_ok))
        def _():
            sx[pl.ds(out0, REACH)] = jnp.zeros((REACH, pp, dm), BF16)

    def normalize():
        need_own(0)
        need_own(2 + len(GROUPS))
        for v in range(nv):
            gx[v, block(me), :] = norm_rows(raw[v], tgain[...])

    lane_h = lax.broadcasted_iota(jnp.int32, (1, hw), 1) // HD
    blk = full // 2

    def time_of(v):
        need(("tr", v), pp)
        need_own(1)
        need("mk", 0, mk.at[pl.ds(0, n - 1)])
        need_own(5 + len(GROUPS))
        seen = jnp.concatenate([mk[s][v:v + 1] for s in range(n)], axis=1)
        normed = gx[v]
        q = dot_t(normed, wt[0:hw, :]).astype(BF16)
        k = dot_t(normed, wt[hw:2 * hw, :]).astype(BF16)
        val = dot_t(normed, wt[2 * hw:3 * hw, :]).astype(BF16)
        qs = [q * jnp.where(lane_h == h, HD ** (-0.5), 0.0).astype(BF16) for h in range(heads)]
        todo = [(b, h) for b in range(2) for h in range(heads)]
        allowed = []
        for b in range(2):
            keys = (b + 1) * blk
            qi = lax.broadcasted_iota(jnp.int32, (blk, keys), 0) + b * blk
            ki = lax.broadcasted_iota(jnp.int32, (blk, keys), 1)
            allowed.append(((ki < qi) & (seen[:, :keys] > 0)) | (ki == qi))
        ss = [dot_t(qs[h][b * blk:(b + 1) * blk], k[:(b + 1) * blk]) for b, h in todo]
        ss = [jnp.where(allowed[b], s, -jnp.inf) for (b, h), s in zip(todo, ss)]
        tops = [jnp.max(s, axis=-1, keepdims=True) for s in ss]
        es = [jnp.exp(s - m) for s, m in zip(ss, tops)]
        dens = [1.0 / jnp.sum(e, axis=-1, keepdims=True) for e in es]
        ws = [(e * d).astype(BF16) for e, d in zip(es, dens)]
        os = [dot(w, val[:(b + 1) * blk]) for (b, h), w in zip(todo, ws)]
        for b in range(2):
            res = os[b * heads]
            for h in range(1, heads):
                res = jnp.where(lane_h == h, os[b * heads + h], res)
            att[v, b * blk:(b + 1) * blk, :] = res[:, :wide].astype(BF16)
            tail = res[:, wide:]
            for i in range(blk // pp):
                lo = b * blk + i * pp
                pair = jnp.concatenate([tail[i * pp:i * pp + half], tail[i * pp + half:(i + 1) * pp]], axis=1)
                att_b[v, lo // 2:lo // 2 + half, :] = pair.astype(BF16)
        for d in (2, 0, 1):
            push("x", att.at[v, block(side[d]), :], ratt.at[me, v], ("a", v), pp * hw // dm, patch=side[d])
            at = pl.ds(pl.multiple_of(side[d] * half, half), half)
            push("x", att_b.at[v, at, :], ratt_b.at[me, v], ("a", v), 0, patch=side[d])
        ratt[me, v] = att[v, block(me), :]
        ratt_b[me, v] = att_b[v, pl.ds(pl.multiple_of(me * half, half), half), :]

    def middle_of(v):
        need(("a", v), (n - 1) * pp * hw // dm)
        for j in (0, 1, 3):
            have("ot", j)
        mix = jnp.zeros((pp, dm), F32)
        for s in range(n):
            pair = ratt_b[s, v]
            tail = jnp.concatenate([pair[:, :hw - wide], pair[:, hw - wide:]], axis=0)
            mix = mix + dot(jnp.concatenate([ratt[s, v], tail], axis=1), wall[base("ot", s):base("ot", s) + hw, :])
        need_own(3 + len(GROUPS))
        middle = (raw[v].astype(F32) + mix).astype(BF16)
        mid[v * pp:(v + 1) * pp, :] = middle
        sx[own0 + v] = norm_rows(middle, sgain[...])

        @pl.when(near_ok)
        def _():
            push("near", sx.at[own0 + v], sx.at[3 - core + v], "near", pp, var=near)

        @pl.when(far_ok & (v - 1 + core >= 0) & (v - 1 + core < 2))
        def _():
            push("far", sx.at[own0 + v], sx.at[7 * core + v - 1], "far", pp, var=far)

    def halo():
        if "halo" in waited:
            return
        waited.add("halo")

        @pl.when(near_ok)
        def _():
            drain(recv.at[names["near"]], nv * pp)
            drain(recv.at[names["far"]], 2 * pp)

    def weight(g):
        for j in (0, 1, 3):
            have(g, j)
        return wall[base(g, 0):base(g, n), :]

    def pass_on(g, name, src, dst, num):
        t = "kv".index(g)
        push("x", kv.at[t, pl.ds(src, num)], kv.at[t, pl.ds(dst, num)], (name, g), num * pp, var=sib)

    def own_part(g):
        x = sx[pl.ds(own0, nv)].reshape(rows, dm)
        part = dot_t(x, weight(g)).astype(BF16)
        if g == "q":
            qb[...] = part * jnp.asarray(HD ** (-0.5), BF16)
        else:
            kv["kv".index(g), REACH:REACH + nv] = part.reshape(nv, pp, dm)
            pass_on(g, "ko", REACH, REACH - nv + 2 * nv * core, nv)

    def halo_part(g):
        halo()
        x = sx[pl.ds(out0, REACH)].reshape(REACH * pp, dm)
        part = dot_t(x, weight(g)).astype(BF16)
        kv["kv".index(g), pl.ds(core * (REACH + nv), REACH)] = part.reshape(REACH, pp, dm)
        pass_on(g, "kh", REACH - 2 + (nv + 2) * core, (REACH + 2 * nv) * core, REACH - nv)

    lane_k = lax.broadcasted_iota(jnp.int32, (1, KEYS), 1) // HD
    pack = KEYS // HD

    def space(which):
        for g in "kv":
            need(("ko", g), nv * pp)
            need(("kh", g), (REACH - nv) * pp)
        bias = jnp.concatenate([mask[...]] * pack, axis=0)
        blank = jnp.zeros((KEYS - slots * TILE, KEYS), BF16)
        num = nv * TILE
        todo = [(b, c) for b in range(2 * which, 2 * which + 2) for c in range(dm // KEYS)]

        def picks(t, b, on):
            at = slice(b * TILE, (b + 1) * TILE)
            return jnp.concatenate([kv[t, i, at, on] for i in range(slots)] + [blank], axis=0)

        for lo in range(0, len(todo), BATCH):
            part = todo[lo:lo + BATCH]
            ss = []
            for b, c in part:
                on = slice(c * KEYS, (c + 1) * KEYS)
                q = jnp.concatenate([qb[u * pp + b * TILE:u * pp + (b + 1) * TILE, on] for u in range(nv)], axis=0)
                many = jnp.concatenate([q * (lane_k == h).astype(F32).astype(BF16) for h in range(pack)], axis=0)
                ss.append(dot_t(many, picks(0, b, on)) + bias)
            tops = [jnp.max(s, axis=-1, keepdims=True) for s in ss]
            es = [jnp.exp(s - m) for s, m in zip(ss, tops)]
            dens = [1.0 / jnp.sum(e, axis=-1, keepdims=True) for e in es]
            ws = [(e * d).astype(BF16) for e, d in zip(es, dens)]
            for (b, c), w in zip(part, ws):
                on = slice(c * KEYS, (c + 1) * KEYS)
                o = dot(w, picks(1, b, on))
                res = o[:num]
                for h in range(1, pack):
                    res = jnp.where(lane_k == h, o[h * num:(h + 1) * num], res)
                res = res.astype(BF16)
                for u in range(nv):
                    att2[u * pp + b * TILE:u * pp + (b + 1) * TILE, on] = res[u * TILE:(u + 1) * TILE]

    def finish():
        total = mid[...].astype(F32) + dot(att2[...], weight("os"))
        out[...] = total.astype(BF16).reshape(nv, pp, dm)

    for d in range(3):
        push("mk", marks, mk.at[me], "mk", 0, patch=side[d])
    steps = {"D": w_direct, "R": w_relay, "Z": w_mate, "G": w_diag}
    calls = {"t": tokens, "tr": tokens_relay, "c": time_of, "m": middle_of, "S": space}
    parts = {"A": own_part, "H": halo_part}
    once = {"init": init, "n": normalize, "O": finish}
    for step in PLAN:
        if step in once:
            once[step]()
        elif step[0] in parts:
            parts[step[0]](step[1])
        elif ":" in step:
            g, what = step.split(":")
            if what in steps:
                steps[what](g)
            else:
                w_share(g, "TU".index(what))
        else:
            calls[step[:-1]](int(step[-1]))

    for i in range(len(own)):
        need_own(i)
    drain(send.at[0], sent["w"])
    drain(send.at[1], sent["x"])
    settle(send.at[2], mk.at[pl.ds(0, n - 1)])

    @pl.when(near_ok)
    def _():
        drain(send.at[3], nv * pp)

    @pl.when(far_ok)
    def _():
        drain(send.at[4], 2 * pp)


def on_device(n, nvar, tokens, patch_mask, group_ids, time_gain, time_qkv, time_out, space_gain, space_qkv, space_out):
    pp, nv, dm = tokens.shape
    hw = time_out.shape[0]
    tok = jnp.transpose(tokens, (1, 0, 2))
    wt = jnp.transpose(time_qkv, (1, 2, 0)).reshape(3 * hw, dm)
    wqs = jnp.transpose(space_qkv, (1, 2, 0)).reshape(3 * hw, dm)
    vm = pl.BlockSpec(memory_space=pltpu.VMEM)
    anyv = pl.BlockSpec(memory_space=pltpu.HBM)
    dma = pltpu.SemaphoreType.DMA
    res = pl.pallas_call(
        functools.partial(kernel, n, nvar),
        out_shape=jax.ShapeDtypeStruct((nv, pp, dm), BF16),
        in_specs=[anyv] * 9,
        out_specs=vm,
        scratch_shapes=[
            pltpu.VMEM((nv, n * pp, dm), BF16),
            pltpu.VMEM((nv, pp, dm), BF16),
            pltpu.VMEM((n, nv, pp), jnp.int32),
            pltpu.VMEM((3 * hw, dm), BF16),
            pltpu.VMEM((5 * n * hw, dm), BF16),
            pltpu.VMEM((nv, n * pp, 2 * HD), BF16),
            pltpu.VMEM((nv, n * pp // 2, 2 * HD), BF16),
            pltpu.VMEM((n, nv, pp, 2 * HD), BF16),
            pltpu.VMEM((n, nv, pp // 2, 2 * HD), BF16),
            pltpu.VMEM((nv * pp, dm), BF16),
            pltpu.VMEM((REACH + nv, pp, dm), BF16),
            pltpu.VMEM((2, 2 * REACH + nv, pp, dm), BF16),
            pltpu.VMEM((nv * pp, dm), BF16),
            pltpu.VMEM((nv * TILE, KEYS), F32),
            pltpu.VMEM((nv * pp, dm), BF16),
            pltpu.SMEM(group_ids.shape, jnp.int32),
            pltpu.VMEM((dm,), F32),
            pltpu.VMEM((dm,), F32),
            dma((6 + len(GROUPS),)), dma((len(sem_names(nv)),)), dma((5,)),
        ],
        compiler_params=pltpu.CompilerParams(
            collective_id=0, has_side_effects=True, vmem_limit_bytes=56_200_000
        ),
    )(tok, patch_mask.T, group_ids, time_gain, space_gain, wt, time_out, wqs, space_out)
    return jnp.transpose(res, (1, 0, 2))


def solution(mesh):
    in_specs = (
        P("patch", ("parts", "var"), None),
        P("patch", ("parts", "var")),
        P("parts"),
        P(),
        P(None, None, "patch"),
        P("patch", None),
        P(),
        P(None, None, "patch"),
        P("patch", None),
    )
    out_specs = P("patch", ("parts", "var"), None)
    return jax.shard_map(
        functools.partial(on_device, mesh.shape["patch"], mesh.shape["var"]),
        mesh=mesh, in_specs=in_specs, out_specs=out_specs, check_vma=False,
    )
```
